32 devices in a mesh: dp: 1 (over z), cpo: 4 (over y), cpi: 8 (over x, core).
Axes of the slice: x: 4, y: 4, z: 1, core: 2. Of those that a mesh axis runs over, the one named last changes fastest.
The devices are a block of a 4x4x8 slice.
Arguments:
- hidden: bfloat16 [8192, 4096], P(('dp', 'cpo', 'cpi'))
- w_query: bfloat16 [4096, 32, 128], replicated
- w_key: bfloat16 [4096, 8, 128], replicated
- w_value: bfloat16 [4096, 8, 128], replicated
- w_out: bfloat16 [32, 128, 4096], replicated
Outputs:
- output: bfloat16 [8192, 4096], P(('dp', 'cpo', 'cpi'))
All inputs are finite; a program needn't handle non-finite values.
Results may differ from the reference program's by a relative error of at most 0.00596079.
Values are sent between devices in bfloat16 or wider.
A program may use at most 768 MiB of HBM per device.

```python
import jax
import jax.numpy as jnp
from jax import lax

MODEL_DIM = 4096
Q_HEADS = 32
KV_HEADS = 8
HEAD_DIM = 128
TOK_DEV = 256
OUTER_DEVS = 4
INNER_DEVS = 8
ROPE_BASE = 500000.0


def token_positions():
    n_dev = OUTER_DEVS * INNER_DEVS
    chunk_len = TOK_DEV // 2
    row_ids = jnp.arange(n_dev * TOK_DEV, dtype=jnp.int32)
    owner_dev = row_ids // TOK_DEV
    second_half = (row_ids // chunk_len) % 2
    chunk_idx = jnp.where(second_half == 0, owner_dev, 2 * n_dev - 1 - owner_dev)
    return chunk_idx * chunk_len + row_ids % chunk_len


def rope_tables(positions):
    half_dim = HEAD_DIM // 2
    inv_freq = ROPE_BASE ** (-(2.0 / HEAD_DIM) * jnp.arange(half_dim, dtype=jnp.float32))
    angles = positions.astype(jnp.float32)[:, None] * inv_freq[None, :]
    return jnp.cos(angles), jnp.sin(angles)


def apply_rope(proj_in, cos_b, sin_b):
    half_dim = proj_in.shape[-1] // 2
    lower_half = proj_in[..., :half_dim]
    upper_half = proj_in[..., half_dim:]
    return jnp.concatenate([lower_half * cos_b - upper_half * sin_b, upper_half * cos_b + lower_half * sin_b], axis=-1)


def setup_inputs(seed: int = 0, part: int = 0) -> dict:
    n_dev = OUTER_DEVS * INNER_DEVS
    seq_len = n_dev * TOK_DEV
    chunk_len = TOK_DEV // 2
    root_key = jax.random.key(seed)
    part_root, shared_root = jax.random.split(root_key)
    part_key = jax.random.fold_in(part_root, part)
    noise_key, chunk_key = jax.random.split(part_key)
    wq_key, wk_key, wv_key, wo_key = jax.random.split(shared_root, 4)
    chunk_means = jax.random.normal(chunk_key, (2 * n_dev, MODEL_DIM), jnp.float32)
    chunk_of_row = token_positions() // chunk_len
    noise_rows = jax.random.normal(noise_key, (seq_len, MODEL_DIM), jnp.float32)
    hidden = 0.6 * noise_rows + chunk_means[chunk_of_row]
    in_scale = MODEL_DIM ** -0.5
    out_scale = (Q_HEADS * HEAD_DIM) ** -0.5
    w_query = jax.random.normal(wq_key, (MODEL_DIM, Q_HEADS, HEAD_DIM), jnp.float32) * in_scale
    w_key = jax.random.normal(wk_key, (MODEL_DIM, KV_HEADS, HEAD_DIM), jnp.float32) * in_scale
    w_value = jax.random.normal(wv_key, (MODEL_DIM, KV_HEADS, HEAD_DIM), jnp.float32) * in_scale
    w_out = jax.random.normal(wo_key, (Q_HEADS, HEAD_DIM, MODEL_DIM), jnp.float32) * out_scale
    return dict(hidden=hidden.astype(jnp.bfloat16), w_query=w_query.astype(jnp.bfloat16), w_key=w_key.astype(jnp.bfloat16), w_value=w_value.astype(jnp.bfloat16), w_out=w_out.astype(jnp.bfloat16))


def reference(hidden, w_query, w_key, w_value, w_out):
    n_dev = OUTER_DEVS * INNER_DEVS
    seq_len = n_dev * TOK_DEV
    n_chunks = 2 * n_dev
    chunk_len = TOK_DEV // 2
    group_size = Q_HEADS // KV_HEADS
    score_scale = HEAD_DIM ** -0.5
    positions = token_positions()
    cos_t, sin_t = rope_tables(positions)
    cos_b = cos_t[:, None, :]
    sin_b = sin_t[:, None, :]
    q_proj = jnp.dot(hidden, w_query.reshape(MODEL_DIM, Q_HEADS * HEAD_DIM), preferred_element_type=jnp.float32)
    k_proj = jnp.dot(hidden, w_key.reshape(MODEL_DIM, KV_HEADS * HEAD_DIM), preferred_element_type=jnp.float32)
    v_proj = jnp.dot(hidden, w_value.reshape(MODEL_DIM, KV_HEADS * HEAD_DIM), preferred_element_type=jnp.float32)
    queries = apply_rope(q_proj.reshape(seq_len, Q_HEADS, HEAD_DIM), cos_b, sin_b).astype(jnp.bfloat16)
    keys_rot = apply_rope(k_proj.reshape(seq_len, KV_HEADS, HEAD_DIM), cos_b, sin_b).astype(jnp.bfloat16)
    values_bf = v_proj.reshape(seq_len, KV_HEADS, HEAD_DIM).astype(jnp.bfloat16)
    q_heads = queries.astype(jnp.float32).reshape(n_chunks, chunk_len, KV_HEADS, group_size, HEAD_DIM).transpose(2, 0, 3, 1, 4)
    k_heads = keys_rot.astype(jnp.float32).transpose(1, 0, 2)
    v_heads = values_bf.astype(jnp.float32).transpose(1, 0, 2)
    q_pos = positions.reshape(n_chunks, chunk_len)

    def one_head(head_args):
        q_head, k_head, v_head = head_args

        def one_chunk(chunk_args):
            q_chunk, pos_chunk = chunk_args
            scores = jnp.einsum('gqd,sd->gqs', q_chunk, k_head) * score_scale
            causal = positions[None, None, :] <= pos_chunk[None, :, None]
            scores = jnp.where(causal, scores, -jnp.inf)
            probs_blk = jax.nn.softmax(scores, axis=-1)
            return jnp.einsum('gqs,sd->gqd', probs_blk, v_head)

        return lax.map(one_chunk, (q_head, q_pos))

    attn_rows = lax.map(one_head, (q_heads, k_heads, v_heads))
    attn_rows = attn_rows.transpose(1, 3, 0, 2, 4).reshape(seq_len, Q_HEADS * HEAD_DIM).astype(jnp.bfloat16)
    out_rows = jnp.dot(attn_rows, w_out.reshape(Q_HEADS * HEAD_DIM, MODEL_DIM), preferred_element_type=jnp.float32)
    return out_rows.astype(jnp.bfloat16)
```

```python
import functools

import jax
import jax.numpy as jnp
from jax import lax
from jax.experimental import pallas as pl
from jax.experimental.pallas import tpu as pltpu
from jax.sharding import PartitionSpec as P

ROPE_BASE = 500000.0
NEG_BIG = -1e30
LOG2E = 1.4426950408889634
MESH = pl.DeviceIdType.MESH
F32 = jnp.float32
BF16 = jnp.bfloat16


def rope_tables(positions, head_dim):
    half_dim = head_dim // 2
    inv_freq = ROPE_BASE ** (-(2.0 / head_dim) * jnp.arange(half_dim, dtype=F32))
    angles = positions.astype(F32)[..., None] * inv_freq
    return jnp.cos(angles), jnp.sin(angles)


def layer_kernel(n_outer, n_inner, x_ref, cos_ref, sin_ref, wq_ref, wk_ref, wv_ref, wo_ref, out_ref,
                 qk_send, v_send, k_all, v_all, q_all, o_stage, o_all,
                 w_sem, send_k, recv_k, send_v, recv_v, send_q, recv_q, send_o, recv_o, send_y, recv_y):
    outer = lax.axis_index("cpo")
    inner = lax.axis_index("cpi")
    rows, model = x_ref.shape
    chunk = rows // 2
    hd = cos_ref.shape[1]
    block = n_inner * chunk
    n_blocks = 2 * n_outer
    groups = wq_ref.shape[1] // n_inner
    per_kv = groups
    tile = 2 * chunk
    n_tiles = block // tile
    cols = per_kv * tile
    scale = LOG2E * hd ** -0.5
    up = lax.rem(outer + 1, n_outer)
    down = lax.rem(outer + n_outer - 1, n_outer)
    far = lax.rem(outer + 2, n_outer)
    mirror = n_blocks - 1

    def across(peer):
        return {"cpi": peer}

    def along(peer):
        return {"cpo": peer}

    def landed(ref, sem):
        pltpu.make_async_copy(ref, ref, sem).wait()

    barrier = pltpu.get_barrier_semaphore()
    for d in range(1, n_inner):
        pl.semaphore_signal(barrier, inc=1, device_id=across(lax.rem(inner + d, n_inner)), device_id_type=MESH)
    for peer in (up, down):
        pl.semaphore_signal(barrier, inc=1, device_id=along(peer), device_id_type=MESH)

    def half_block(half, owner_outer):
        return owner_outer if half == 0 else mirror - owner_outer

    def half_rows(half, who):
        start = who * chunk if half == 0 else (n_inner - 1 - who) * chunk
        return pl.ds(pl.multiple_of(start, chunk), chunk)

    def k_copy(half, peer, owner, sem_peer):
        return dict(src_ref=qk_send.at[half, peer], dst_ref=k_all.at[half_block(half, outer), half_rows(half, owner), :])

    def v_copy(half, peer, owner):
        return dict(src_ref=v_send.at[half, peer], dst_ref=v_all.at[half_block(half, outer), :, half_rows(half, owner)])

    def q_copy(half, peer, owner):
        heads = pl.ds(n_inner + peer * per_kv, per_kv)
        return dict(src_ref=qk_send.at[half, heads], dst_ref=q_all.at[half, :, half_rows(half, owner), :])

    def exchange(make, send, recv, peer):
        @pl.when(peer != inner)
        def _():
            for half in range(2):
                refs = make(half, peer, inner)
                pltpu.make_async_remote_copy(send_sem=send.at[half, peer], recv_sem=recv.at[half, inner],
                                             device_id=across(peer), device_id_type=MESH, **refs).start()

        @pl.when(peer == inner)
        def _():
            for half in range(2):
                refs = make(half, peer, inner)
                pltpu.make_async_copy(refs["src_ref"], refs["dst_ref"], recv.at[half, inner]).start()

    def kv_landed():
        def one(src, _):
            for half in range(2):
                landed(k_all.at[half_block(half, outer), half_rows(half, src), :], recv_k.at[half, src])
                landed(v_all.at[half_block(half, outer), :, half_rows(half, src)], recv_v.at[half, src])
            return 0
        lax.fori_loop(0, n_inner, one, 0)

    def y_parts(src):
        return (k_all.at[src], k_all.at[mirror - src], v_all.at[src], v_all.at[mirror - src])

    def y_send(src, part, slot, lane, peer):
        ref = y_parts(src)[part]
        return pltpu.make_async_remote_copy(src_ref=ref, dst_ref=ref, send_sem=send_y.at[slot, part],
                                            recv_sem=recv_y.at[lane, part], device_id=along(peer), device_id_type=MESH)

    def project(w_buf, y_buf):
        def fetch(e, do):
            slot = lax.rem(e, 2)

            @pl.when(e == 0)
            def _():
                do(pltpu.make_async_copy(wk_ref, w_buf.at[slot], w_sem.at[slot]))

            @pl.when(e == 1)
            def _():
                do(pltpu.make_async_copy(wv_ref, w_buf.at[slot], w_sem.at[slot]))

            @pl.when(e >= 2)
            def _():
                heads = pl.ds(pl.multiple_of(group_of(e) * n_inner, n_inner), n_inner)
                do(pltpu.make_async_copy(wq_ref.at[:, heads, :], w_buf.at[slot], w_sem.at[slot]))

        def group_of(e):
            return lax.rem(inner * groups // n_inner + e, groups)

        fetch(0, lambda c: c.start())
        fetch(1, lambda c: c.start())
        pl.semaphore_wait(barrier, n_inner + 1)

        def step(e, _):
            slot = lax.rem(e, 2)
            fetch(e, lambda c: c.wait())
            y_buf[...] = jnp.dot(x_ref[...], w_buf[slot].reshape(model, n_inner * hd), preferred_element_type=F32)

            @pl.when(e + 2 < groups + 2)
            def _():
                fetch(e + 2, lambda c: c.start())

            @pl.when(e == 1)
            def _():
                for h in range(n_inner):
                    vt = y_buf[:, h * hd:(h + 1) * hd].T.astype(BF16)
                    for half in range(2):
                        v_send[half, h] = vt[:, half * chunk:(half + 1) * chunk]

                def one(d, _):
                    exchange(v_copy, send_v, recv_v, lax.rem(inner + d, n_inner))
                    return 0
                lax.fori_loop(0, n_inner, one, 0)

            @pl.when(e != 1)
            def _():
                base = jnp.where(e == 0, 0, n_inner + group_of(e) * n_inner)
                for h in range(n_inner):
                    y = y_buf[:, h * hd:(h + 1) * hd]
                    r = (y * cos_ref[...] + pltpu.roll(y, hd // 2, 1) * sin_ref[...]).astype(BF16)
                    for half in range(2):
                        qk_send[half, base + h] = r[half * chunk:(half + 1) * chunk]

            @pl.when(e == 0)
            def _():
                def one(d, _):
                    exchange(functools.partial(k_copy, sem_peer=None), send_k, recv_k, lax.rem(inner + d, n_inner))
                    return 0
                lax.fori_loop(0, n_inner, one, 0)

            @pl.when(e >= 2)
            def _():
                first = group_of(e) * (n_inner // groups)

                def one(d, _):
                    exchange(q_copy, send_q, recv_q, first + d)
                    return 0
                lax.fori_loop(0, n_inner // groups, one, 0)
            return 0
        lax.fori_loop(0, groups + 2, step, 0)

    pl.run_scoped(project, pltpu.VMEM((2, model, n_inner, hd), BF16), pltpu.VMEM((rows, n_inner * hd), F32))

    kv_landed()
    for part in range(4):
        y_send(outer, part, 0, 0, up).start()
        y_send(outer, part, 1, 1, down).start()

    def attend(w_buf, s0, s1, qt, m_buf, l_buf, acc):
        wide = w_buf.shape[2]

        def out_weights(c, slot):
            return pltpu.make_async_copy(wo_ref.at[:, pl.ds(pl.multiple_of(c * wide, wide), wide)], w_buf.at[slot], w_sem.at[slot])

        for c in range(2):
            out_weights(c, c).start()

        def q_landed(src, _):
            for half in range(2):
                landed(q_all.at[half, :, half_rows(half, src), :], recv_q.at[half, src])
            return 0
        lax.fori_loop(0, n_inner, q_landed, 0)

        def qk(s_buf, unit):
            side, t, kb, _ = unit
            s_buf[...] = jnp.dot(k_all[kb], qt[side * n_tiles + t], preferred_element_type=F32)

        def soft(s_buf, unit):
            side, t, kb, masked = unit
            idx = side * n_tiles + t
            s = s_buf[...]
            if masked:
                key = lax.broadcasted_iota(jnp.int32, s.shape, 0)
                pos = lax.rem(lax.broadcasted_iota(jnp.int32, s.shape, 1), tile) + t * tile
                s = jnp.where(key <= pos, s, NEG_BIG)
            m_old = m_buf[idx]
            m_new = jnp.maximum(m_old, s.max(axis=0, keepdims=True))
            p = jnp.exp2((s - m_new) * scale)
            rescale = jnp.exp2((m_old - m_new) * scale)
            m_buf[idx] = m_new
            l_buf[idx] = l_buf[idx] * rescale + p.sum(axis=0, keepdims=True)
            acc[idx] = acc[idx] * rescale + jnp.dot(v_all[kb], p.astype(BF16), preferred_element_type=F32)

        def run(units):
            bufs = (s0, s1)
            qk(bufs[0], units[0])
            for n, unit in enumerate(units):
                if n + 1 < len(units):
                    qk(bufs[(n + 1) % 2], units[n + 1])
                soft(bufs[n % 2], unit)

        def own(t, _):
            for side in range(2):
                idx = side * n_tiles + t
                for h in range(per_kv):
                    piece = q_all[side, h, pl.ds(pl.multiple_of(t * tile, tile), tile), :]
                    qt[idx, :, h * tile:(h + 1) * tile] = piece.T
                m_buf[idx] = jnp.full((1, cols), NEG_BIG, F32)
                l_buf[idx] = jnp.zeros((1, cols), F32)
                acc[idx] = jnp.zeros((hd, cols), F32)
            run([(0, t, outer, True), (1, t, mirror - outer, True), (1, t, outer, False)])
            return 0
        lax.fori_loop(0, n_tiles, own, 0)

        for part in range(4):
            landed(y_parts(down)[part], recv_y.at[0, part])
            landed(y_parts(up)[part], recv_y.at[1, part])
        for part in range(2):
            y_send(down, part, 2, 2, up).start()
            y_send(up, part + 2, 2, 2, down).start()

        def source(src, t):
            earlier = src < outer
            return [(jnp.where(earlier, 0, 1), t, src, False), (1, t, jnp.where(earlier, src, mirror - src), False)]

        def neighbour(t, _):
            run(source(down, t))
            return 0
        lax.fori_loop(0, n_tiles, neighbour, 0)

        for part in range(4):
            landed(y_parts(far)[part], recv_y.at[2, part])

        def o_copy(half, t, j):
            c = 2 * t + j
            peer = c if half == 0 else n_inner - 1 - c
            src = o_stage.at[half, t, pl.ds(j * chunk, chunk), :]
            dst = o_all.at[pl.ds(half * chunk, chunk), pl.ds(pl.multiple_of(inner * per_kv * hd, per_kv * hd), per_kv * hd)]
            return peer, src, dst

        def last(t, _):
            run(source(up, t) + source(far, t))
            for half in range(2):
                idx = half * n_tiles + t
                o_t = acc[idx] / l_buf[idx]
                for h in range(per_kv):
                    o_stage[half, t, :, h * hd:(h + 1) * hd] = o_t[:, h * tile:(h + 1) * tile].T.astype(BF16)
                for j in range(2):
                    peer, src, dst = o_copy(half, t, j)

                    @pl.when(peer != inner)
                    def _():
                        pltpu.make_async_remote_copy(src_ref=src, dst_ref=dst, send_sem=send_o.at[half, peer],
                                                     recv_sem=recv_o.at[half, inner], device_id=across(peer),
                                                     device_id_type=MESH).start()

                    @pl.when(peer == inner)
                    def _():
                        pltpu.make_async_copy(src, dst, recv_o.at[half, inner]).start()
            return 0
        lax.fori_loop(0, n_tiles, last, 0)

        def o_landed(src, _):
            for half in range(2):
                landed(o_all.at[pl.ds(half * chunk, chunk), pl.ds(pl.multiple_of(src * per_kv * hd, per_kv * hd), per_kv * hd)],
                       recv_o.at[half, src])
            return 0
        lax.fori_loop(0, n_inner, o_landed, 0)
        n_wide = model // wide

        def out_step(c, _):
            slot = lax.rem(c, 2)
            out_weights(c, slot).wait()
            res = jnp.dot(o_all[...], w_buf[slot], preferred_element_type=F32)
            out_ref[:, pl.ds(pl.multiple_of(c * wide, wide), wide)] = res.astype(BF16)

            @pl.when(c + 2 < n_wide)
            def _():
                out_weights(c + 2, slot).start()
            return 0
        lax.fori_loop(0, n_wide, out_step, 0)

        def sent(d, _):
            peer = lax.rem(inner + d, n_inner)
            heads = pl.ds(n_inner + peer * per_kv, per_kv)
            for half in range(2):
                landed(qk_send.at[half, peer], send_k.at[half, peer])
                landed(v_send.at[half, peer], send_v.at[half, peer])
                landed(qk_send.at[half, heads], send_q.at[half, peer])
                landed(o_stage.at[half, 0, pl.ds(0, chunk), :], send_o.at[half, peer])
            return 0
        lax.fori_loop(1, n_inner, sent, 0)
        for slot in range(3):
            for part in range(4):
                landed(y_parts(outer)[part], send_y.at[slot, part])

    pl.run_scoped(attend, pltpu.VMEM((2, wo_ref.shape[0], 1024), BF16), pltpu.VMEM((block, cols), F32),
                  pltpu.VMEM((block, cols), F32), pltpu.VMEM((2 * n_tiles, hd, cols), BF16),
                  pltpu.VMEM((2 * n_tiles, 1, cols), F32), pltpu.VMEM((2 * n_tiles, 1, cols), F32),
                  pltpu.VMEM((2 * n_tiles, hd, cols), F32))


def solution(mesh):
    n_outer = mesh.shape['cpo']
    n_inner = mesh.shape['cpi']
    n_dev = n_outer * n_inner

    def device_step(hidden, w_query, w_key, w_value, w_out):
        rows, model = hidden.shape
        chunk = rows // 2
        q_heads, hd = w_query.shape[1:]
        per_kv = q_heads // n_inner
        block = n_inner * chunk
        n_tiles = block // (2 * chunk)
        rank = lax.axis_index('cpo') * n_inner + lax.axis_index('cpi')
        offsets = jnp.arange(chunk, dtype=jnp.int32)
        positions = jnp.concatenate([rank * chunk + offsets, (2 * n_dev - 1 - rank) * chunk + offsets])
        cos, sin = rope_tables(positions, hd)
        cos2 = jnp.concatenate([cos, cos], axis=1)
        sin2 = jnp.concatenate([-sin, sin], axis=1)
        dma = pltpu.SemaphoreType.DMA
        pair = dma((2, n_inner))
        vmem = pl.BlockSpec(memory_space=pltpu.VMEM)
        hbm = pl.BlockSpec(memory_space=pl.ANY)
        return pl.pallas_call(
            functools.partial(layer_kernel, n_outer, n_inner),
            out_shape=jax.ShapeDtypeStruct((rows, model), BF16),
            in_specs=[vmem] * 3 + [hbm] * 4,
            out_specs=vmem,
            scratch_shapes=[
                pltpu.VMEM((2, n_inner + q_heads, chunk, hd), BF16),
                pltpu.VMEM((2, n_inner, hd, chunk), BF16),
                pltpu.VMEM((2 * n_outer, block, hd), BF16),
                pltpu.VMEM((2 * n_outer, hd, block), BF16),
                pltpu.VMEM((2, per_kv, block, hd), BF16),
                pltpu.VMEM((2, n_tiles, 2 * chunk, per_kv * hd), BF16),
                pltpu.VMEM((rows, q_heads * hd), BF16),
                dma((2,)), pair, pair, pair, pair, pair, pair, pair, pair, dma((3, 4)), dma((3, 4)),
            ],
            compiler_params=pltpu.CompilerParams(collective_id=0, has_side_effects=True, vmem_limit_bytes=66 * 1000 * 1000),
        )(hidden, cos2, sin2, w_query, w_key, w_value, w_out.reshape(q_heads * hd, model))

    row_spec = P(('dp', 'cpo', 'cpi'), None)
    weight_spec = P(None, None, None)
    return jax.shard_map(device_step, mesh=mesh, in_specs=(row_spec, weight_spec, weight_spec, weight_spec, weight_spec), out_specs=row_spec, check_vma=False)
```

```python
import functools

import jax
import jax.numpy as jnp
from jax import lax
from jax.experimental import pallas as pl
from jax.experimental.pallas import tpu as pltpu
from jax.sharding import PartitionSpec as P

ROPE_BASE = 500000.0
NEG_BIG = -1e30
LOG2E = 1.4426950408889634
MESH = pl.DeviceIdType.MESH
F32 = jnp.float32
BF16 = jnp.bfloat16


def rope_tables(positions, head_dim):
    half_dim = head_dim // 2
    lane = jnp.arange(head_dim, dtype=jnp.int32)
    inv_freq = ROPE_BASE ** (-(2.0 / head_dim) * (lane % half_dim).astype(F32))
    angles = positions.astype(F32)[:, None] * inv_freq
    return jnp.cos(angles), jnp.where(lane < half_dim, -jnp.sin(angles), jnp.sin(angles))


def layer_kernel(n_outer, n_inner, x_ref, cos_ref, sin_ref, wq_ref, wk_ref, wv_ref, wo_ref, out_ref,
                 qk_send, v_send, k_all, v_all, q_all, o_stage, o_all,
                 w_sem, send_k, recv_k, send_v, recv_v, send_q, recv_q, send_o, recv_o, send_y, recv_y):
    outer = lax.axis_index("cpo")
    inner = lax.axis_index("cpi")
    rows, model = x_ref.shape
    chunk = rows // 2
    hd = cos_ref.shape[1]
    block = n_inner * chunk
    n_blocks = 2 * n_outer
    groups = wq_ref.shape[1] // n_inner
    per_kv = groups
    tile = 2 * chunk
    n_tiles = block // tile
    cols = per_kv * tile
    scale = LOG2E * hd ** -0.5
    up = lax.rem(outer + 1, n_outer)
    down = lax.rem(outer + n_outer - 1, n_outer)
    far = lax.rem(outer + 2, n_outer)
    mirror = n_blocks - 1

    here = inner // (n_inner // groups)

    def beyond(hops):
        return lax.rem(here + hops, groups)

    def across(peer):
        return {"cpi": peer}

    def along(peer):
        return {"cpo": peer}

    def landed(ref, sem):
        pltpu.make_async_copy(ref, ref, sem).wait()

    barrier = pltpu.get_barrier_semaphore()
    for d in range(1, n_inner):
        pl.semaphore_signal(barrier, inc=1, device_id=across(lax.rem(inner + d, n_inner)), device_id_type=MESH)
    for peer in (up, down):
        pl.semaphore_signal(barrier, inc=1, device_id=along(peer), device_id_type=MESH)

    def half_block(half, owner_outer):
        return owner_outer if half == 0 else mirror - owner_outer

    def half_rows(half, who):
        start = who * chunk if half == 0 else (n_inner - 1 - who) * chunk
        return pl.ds(pl.multiple_of(start, chunk), chunk)

    def k_copy(half, peer, owner):
        return dict(src_ref=qk_send.at[half, peer], dst_ref=k_all.at[half_block(half, outer), half_rows(half, owner), :])

    def v_copy(half, peer, owner):
        return dict(src_ref=v_send.at[half, peer], dst_ref=v_all.at[half_block(half, outer), :, half_rows(half, owner)])

    def q_copy(half, peer, owner):
        heads = pl.ds(n_inner + peer * per_kv, per_kv)
        return dict(src_ref=qk_send.at[half, heads], dst_ref=q_all.at[half, :, half_rows(half, owner), :])

    def exchange(make, send, recv, peer):
        @pl.when(peer != inner)
        def _():
            for half in range(2):
                refs = make(half, peer, inner)
                pltpu.make_async_remote_copy(send_sem=send.at[half, peer], recv_sem=recv.at[half, inner],
                                             device_id=across(peer), device_id_type=MESH, **refs).start()

        @pl.when(peer == inner)
        def _():
            for half in range(2):
                refs = make(half, peer, inner)
                pltpu.make_async_copy(refs["src_ref"], refs["dst_ref"], recv.at[half, inner]).start()

    def k_landed(src, _):
        for half in range(2):
            landed(k_all.at[half_block(half, outer), half_rows(half, src), :], recv_k.at[half, src])
        return 0

    def v_landed(src, _):
        for half in range(2):
            landed(v_all.at[half_block(half, outer), :, half_rows(half, src)], recv_v.at[half, src])
        return 0

    def y_parts(src):
        return (k_all.at[src], k_all.at[mirror - src], v_all.at[src], v_all.at[mirror - src])

    def y_send(src, part, slot, lane, peer):
        ref = y_parts(src)[part]
        return pltpu.make_async_remote_copy(src_ref=ref, dst_ref=ref, send_sem=send_y.at[slot, part],
                                            recv_sem=recv_y.at[lane, part], device_id=along(peer), device_id_type=MESH)

    def project(w_buf, y_buf):
        def fetch(e, do):
            slot = lax.rem(e, 2)

            @pl.when(e == 0)
            def _():
                do(pltpu.make_async_copy(wk_ref, w_buf.at[slot], w_sem.at[slot]))

            @pl.when(e == 1)
            def _():
                do(pltpu.make_async_copy(wv_ref, w_buf.at[slot], w_sem.at[slot]))

            @pl.when(e >= 2)
            def _():
                heads = pl.ds(pl.multiple_of(group_of(e) * n_inner, n_inner), n_inner)
                do(pltpu.make_async_copy(wq_ref.at[:, heads, :], w_buf.at[slot], w_sem.at[slot]))

        def group_of(e):
            return beyond(jnp.where(e == 2, 1, jnp.where(e == 3, 3, jnp.where(e == 4, 2, 0))))

        fetch(0, lambda c: c.start())
        fetch(1, lambda c: c.start())
        pl.semaphore_wait(barrier, n_inner + 1)

        def step(e, _):
            slot = lax.rem(e, 2)
            fetch(e, lambda c: c.wait())
            y_buf[...] = jnp.dot(x_ref[...], w_buf[slot].reshape(model, n_inner * hd), preferred_element_type=F32)

            @pl.when(e + 2 < groups + 2)
            def _():
                fetch(e + 2, lambda c: c.start())

            @pl.when(e == 1)
            def _():
                for h in range(n_inner):
                    vt = y_buf[:, h * hd:(h + 1) * hd].T.astype(BF16)
                    for half in range(2):
                        v_send[half, h] = vt[:, half * chunk:(half + 1) * chunk]

                def one(d, _):
                    exchange(v_copy, send_v, recv_v, lax.rem(inner + d, n_inner))
                    return 0
                lax.fori_loop(0, n_inner, one, 0)

            @pl.when(e != 1)
            def _():
                base = jnp.where(e == 0, 0, n_inner + group_of(e) * n_inner)
                for h in range(n_inner):
                    y = y_buf[:, h * hd:(h + 1) * hd]
                    r = (y * cos_ref[...] + pltpu.roll(y, hd // 2, 1) * sin_ref[...]).astype(BF16)
                    for half in range(2):
                        qk_send[half, base + h] = r[half * chunk:(half + 1) * chunk]

            @pl.when(e == 0)
            def _():
                def one(d, _):
                    exchange(k_copy, send_k, recv_k, lax.rem(inner + d, n_inner))
                    return 0
                lax.fori_loop(0, n_inner, one, 0)

            @pl.when(e >= 2)
            def _():
                first = group_of(e) * (n_inner // groups)

                def one(d, _):
                    exchange(q_copy, send_q, recv_q, first + d)
                    return 0
                lax.fori_loop(0, n_inner // groups, one, 0)

            for when, here_yet, parts in ((3, k_landed, (0, 1)), (4, v_landed, (2, 3))):
                @pl.when(e == when)
                def _():
                    lax.fori_loop(0, n_inner, here_yet, 0)
                    for part in parts:
                        y_send(outer, part, 0, 0, up).start()
                        y_send(outer, part, 1, 1, down).start()
            return 0
        lax.fori_loop(0, groups + 2, step, 0)

    pl.run_scoped(project, pltpu.VMEM((2, model, n_inner, hd), BF16), pltpu.VMEM((rows, n_inner * hd), F32))

    def attend(w_buf, s0, s1, qt, m_buf, l_buf, acc):
        wide = w_buf.shape[2]

        def out_weights(c, slot):
            return pltpu.make_async_copy(wo_ref.at[:, pl.ds(pl.multiple_of(c * wide, wide), wide)], w_buf.at[slot], w_sem.at[slot])

        for c in range(2):
            out_weights(c, c).start()

        def qk(s_buf, unit):
            side, t, kb, quarter = unit
            if quarter is None:
                s_buf[...] = jnp.dot(k_all[kb], qt[side * n_tiles + t], preferred_element_type=F32)
            else:
                keys = pl.ds(pl.multiple_of(quarter * tile, tile), tile)
                s_buf[:tile] = jnp.dot(k_all[kb, keys, :], qt[side * n_tiles + t], preferred_element_type=F32)

        def soft(s_buf, unit):
            side, t, kb, quarter = unit
            idx = side * n_tiles + t
            if quarter is None:
                s, v = s_buf[...], v_all[kb]
            else:
                keys = pl.ds(pl.multiple_of(quarter * tile, tile), tile)
                s, v = s_buf[:tile], v_all[kb, :, keys]
                key = lax.broadcasted_iota(jnp.int32, s.shape, 0) + (quarter - t) * tile
                pos = lax.rem(lax.broadcasted_iota(jnp.int32, s.shape, 1), tile)
                s = jnp.where(key <= pos, s, NEG_BIG)
            m_old = m_buf[idx]
            m_new = jnp.maximum(m_old, s.max(axis=0, keepdims=True))
            p = jnp.exp2((s - m_new) * scale)
            rescale = jnp.exp2((m_old - m_new) * scale)
            m_buf[idx] = m_new
            l_buf[idx] = l_buf[idx] * rescale + p.sum(axis=0, keepdims=True)
            acc[idx] = acc[idx] * rescale + jnp.dot(v, p.astype(BF16), preferred_element_type=F32)

        def run(units, before=None):
            bufs = (s0, s1)
            qk(bufs[0], units[0])
            for n, unit in enumerate(units):
                if n + 1 < len(units):
                    if before and n + 1 in before:
                        before[n + 1]()
                    qk(bufs[(n + 1) % 2], units[n + 1])
                soft(bufs[n % 2], unit)

        def own(step, _):
            chip = beyond(jnp.where(step == 2, 3, jnp.where(step == 3, 2, step)))
            t_side = (chip, n_tiles - 1 - chip)

            def q_landed(src, _):
                for half in range(2):
                    landed(q_all.at[half, :, half_rows(half, src), :], recv_q.at[half, src])
                return 0
            lax.fori_loop(chip * (n_inner // groups), (chip + 1) * (n_inner // groups), q_landed, 0)

            @pl.when(step == 2)
            def _():
                for part in (0, 1):
                    landed(y_parts(down)[part], recv_y.at[0, part])
                    y_send(down, part, 2, 2, up).start()

            @pl.when(step == 3)
            def _():
                for part in (2, 3):
                    landed(y_parts(up)[part], recv_y.at[1, part])
                    y_send(up, part, 2, 2, down).start()

            for side in range(2):
                t = t_side[side]
                idx = side * n_tiles + t
                for h in range(per_kv):
                    piece = q_all[side, h, pl.ds(pl.multiple_of(t * tile, tile), tile), :]
                    qt[idx, :, h * tile:(h + 1) * tile] = piece.T
                m_buf[idx] = jnp.full((1, cols), NEG_BIG, F32)
                l_buf[idx] = jnp.zeros((1, cols), F32)
                acc[idx] = jnp.zeros((hd, cols), F32)
            units = []
            for n in range(n_tiles + 1):
                front = n <= chip
                units.append((jnp.where(front, 0, 1), jnp.where(front, t_side[0], t_side[1]),
                              jnp.where(front, outer, mirror - outer), jnp.where(front, n, n - chip - 1)))
            run(units + [(1, t_side[1], outer, None)])
            return 0
        lax.fori_loop(0, n_tiles, own, 0)

        for part in (0, 1):
            landed(y_parts(up)[part], recv_y.at[1, part])
        for part in (2, 3):
            landed(y_parts(down)[part], recv_y.at[0, part])

        def source(src, t_side):
            earlier = src < outer
            return [(jnp.where(earlier, 0, 1), jnp.where(earlier, t_side[0], t_side[1]), src, None),
                    (1, t_side[1], jnp.where(earlier, src, mirror - src), None)]

        def o_copy(half, t, j):
            c = 2 * t + j
            peer = c if half == 0 else n_inner - 1 - c
            src = o_stage.at[half, t, pl.ds(j * chunk, chunk), :]
            dst = o_all.at[pl.ds(half * chunk, chunk), pl.ds(pl.multiple_of(inner * per_kv * hd, per_kv * hd), per_kv * hd)]
            return peer, src, dst

        def last(step, _):
            chip = beyond(jnp.where(step == 0, 2, jnp.where(step == 1, 1, jnp.where(step == 2, 3, 0))))
            t_side = (chip, n_tiles - 1 - chip)

            def far_landed():
                @pl.when(step == 0)
                def _():
                    for part in range(4):
                        landed(y_parts(far)[part], recv_y.at[2, part])

            run(source(down, t_side) + source(up, t_side) + source(far, t_side), before={4: far_landed})
            for half in range(2):
                t = t_side[half]
                idx = half * n_tiles + t
                o_t = acc[idx] / l_buf[idx]
                for h in range(per_kv):
                    o_stage[half, t, :, h * hd:(h + 1) * hd] = o_t[:, h * tile:(h + 1) * tile].T.astype(BF16)
                for j in range(2):
                    peer, src, dst = o_copy(half, t, j)

                    @pl.when(peer != inner)
                    def _():
                        pltpu.make_async_remote_copy(src_ref=src, dst_ref=dst, send_sem=send_o.at[half, peer],
                                                     recv_sem=recv_o.at[half, inner], device_id=across(peer),
                                                     device_id_type=MESH).start()

                    @pl.when(peer == inner)
                    def _():
                        pltpu.make_async_copy(src, dst, recv_o.at[half, inner]).start()
            return 0
        lax.fori_loop(0, n_tiles, last, 0)

        def o_landed(src, _):
            for half in range(2):
                landed(o_all.at[pl.ds(half * chunk, chunk), pl.ds(pl.multiple_of(src * per_kv * hd, per_kv * hd), per_kv * hd)],
                       recv_o.at[half, src])
            return 0
        lax.fori_loop(0, n_inner, o_landed, 0)
        n_wide = model // wide

        def out_step(c, _):
            slot = lax.rem(c, 2)
            out_weights(c, slot).wait()
            res = jnp.dot(o_all[...], w_buf[slot], preferred_element_type=F32)
            out_ref[:, pl.ds(pl.multiple_of(c * wide, wide), wide)] = res.astype(BF16)

            @pl.when(c + 2 < n_wide)
            def _():
                out_weights(c + 2, slot).start()
            return 0
        lax.fori_loop(0, n_wide, out_step, 0)

        def sent(d, _):
            peer = lax.rem(inner + d, n_inner)
            heads = pl.ds(n_inner + peer * per_kv, per_kv)
            for half in range(2):
                landed(qk_send.at[half, peer], send_k.at[half, peer])
                landed(v_send.at[half, peer], send_v.at[half, peer])
                landed(qk_send.at[half, heads], send_q.at[half, peer])
                landed(o_stage.at[half, 0, pl.ds(0, chunk), :], send_o.at[half, peer])
            return 0
        lax.fori_loop(1, n_inner, sent, 0)
        for slot in range(3):
            for part in range(4):
                landed(y_parts(outer)[part], send_y.at[slot, part])

    pl.run_scoped(attend, pltpu.VMEM((2, wo_ref.shape[0], 1024), BF16), pltpu.VMEM((block, cols), F32),
                  pltpu.VMEM((block, cols), F32), pltpu.VMEM((2 * n_tiles, hd, cols), BF16),
                  pltpu.VMEM((2 * n_tiles, 1, cols), F32), pltpu.VMEM((2 * n_tiles, 1, cols), F32),
                  pltpu.VMEM((2 * n_tiles, hd, cols), F32))


def solution(mesh):
    n_outer = mesh.shape['cpo']
    n_inner = mesh.shape['cpi']
    n_dev = n_outer * n_inner

    def device_step(hidden, w_query, w_key, w_value, w_out):
        rows, model = hidden.shape
        chunk = rows // 2
        q_heads, hd = w_query.shape[1:]
        per_kv = q_heads // n_inner
        block = n_inner * chunk
        n_tiles = block // (2 * chunk)
        rank = lax.axis_index('cpo') * n_inner + lax.axis_index('cpi')
        offsets = jnp.arange(chunk, dtype=jnp.int32)
        positions = jnp.concatenate([rank * chunk + offsets, (2 * n_dev - 1 - rank) * chunk + offsets])
        cos, sin = rope_tables(positions, hd)
        dma = pltpu.SemaphoreType.DMA
        pair = dma((2, n_inner))
        vmem = pl.BlockSpec(memory_space=pltpu.VMEM)
        hbm = pl.BlockSpec(memory_space=pl.ANY)
        return pl.pallas_call(
            functools.partial(layer_kernel, n_outer, n_inner),
            out_shape=jax.ShapeDtypeStruct((rows, model), BF16),
            in_specs=[vmem] * 3 + [hbm] * 4,
            out_specs=vmem,
            scratch_shapes=[
                pltpu.VMEM((2, n_inner + q_heads, chunk, hd), BF16),
                pltpu.VMEM((2, n_inner, hd, chunk), BF16),
                pltpu.VMEM((2 * n_outer, block, hd), BF16),
                pltpu.VMEM((2 * n_outer, hd, block), BF16),
                pltpu.VMEM((2, per_kv, block, hd), BF16),
                pltpu.VMEM((2, n_tiles, 2 * chunk, per_kv * hd), BF16),
                pltpu.VMEM((rows, q_heads * hd), BF16),
                dma((2,)), pair, pair, pair, pair, pair, pair, pair, pair, dma((3, 4)), dma((3, 4)),
            ],
            compiler_params=pltpu.CompilerParams(collective_id=0, has_side_effects=True, vmem_limit_bytes=56 * 1024 * 1024),
        )(hidden, cos, sin, w_query, w_key, w_value, w_out.reshape(q_heads * hd, model))

    row_spec = P(('dp', 'cpo', 'cpi'), None)
    weight_spec = P(None, None, None)
    return jax.shard_map(device_step, mesh=mesh, in_specs=(row_spec, weight_spec, weight_spec, weight_spec, weight_spec), out_specs=row_spec, check_vma=False)
```

```python
import functools

import jax
import jax.numpy as jnp
from jax import lax
from jax.experimental import pallas as pl
from jax.experimental.pallas import tpu as pltpu
from jax.sharding import PartitionSpec as P

ROPE_BASE = 500000.0
NEG_BIG = -1e30
LOG2E = 1.4426950408889634
MESH = pl.DeviceIdType.MESH
F32 = jnp.float32
BF16 = jnp.bfloat16


def rope_tables(positions, head_dim):
    half_dim = head_dim // 2
    lane = jnp.arange(head_dim, dtype=jnp.int32)
    inv_freq = ROPE_BASE ** (-(2.0 / head_dim) * (lane % half_dim).astype(F32))
    angles = positions.astype(F32)[:, None] * inv_freq
    return jnp.cos(angles), jnp.where(lane < half_dim, -jnp.sin(angles), jnp.sin(angles))


def layer_kernel(n_outer, n_inner, x_hbm, cos_ref, sin_ref, wq_ref, wk_ref, wv_ref, wo_ref, out_ref,
                 x_ref, qk_send, v_send, k_all, v_all, q_all, o_stage, o_all,
                 w_sem, send_k, recv_k, send_v, recv_v, send_q, recv_q, send_o, recv_o, send_y, recv_y):
    outer = lax.axis_index("cpo")
    inner = lax.axis_index("cpi")
    rows, model = x_hbm.shape
    chunk = rows // 2
    hd = cos_ref.shape[1]
    block = n_inner * chunk
    n_blocks = 2 * n_outer
    groups = wq_ref.shape[1] // n_inner
    per_kv = groups
    tile = 2 * chunk
    n_tiles = block // tile
    cols = per_kv * tile
    piece = 2 * tile
    scale = LOG2E * hd ** -0.5
    up = lax.rem(outer + 1, n_outer)
    down = lax.rem(outer + n_outer - 1, n_outer)
    far = lax.rem(outer + 2, n_outer)
    mirror = n_blocks - 1

    here = inner // (n_inner // groups)

    def beyond(hops):
        return lax.rem(here + hops, groups)

    def across(peer):
        return {"cpi": peer}

    def along(peer):
        return {"cpo": peer}

    def landed(ref, sem):
        pltpu.make_async_copy(ref, ref, sem).wait()

    barrier = pltpu.get_barrier_semaphore()
    for d in range(1, n_inner):
        pl.semaphore_signal(barrier, inc=1, device_id=across(lax.rem(inner + d, n_inner)), device_id_type=MESH)
    for peer in (up, down):
        pl.semaphore_signal(barrier, inc=1, device_id=along(peer), device_id_type=MESH)

    def half_block(half, owner_outer):
        return owner_outer if half == 0 else mirror - owner_outer

    def half_rows(half, who):
        start = who * chunk if half == 0 else (n_inner - 1 - who) * chunk
        return pl.ds(pl.multiple_of(start, chunk), chunk)

    def k_copy(half, peer, owner):
        return dict(src_ref=qk_send.at[half, peer], dst_ref=k_all.at[half_block(half, outer), half_rows(half, owner), :])

    def v_copy(half, peer, owner):
        return dict(src_ref=v_send.at[half, peer], dst_ref=v_all.at[half_block(half, outer), :, half_rows(half, owner)])

    def q_copy(half, peer, owner):
        heads = pl.ds(n_inner + peer * per_kv, per_kv)
        return dict(src_ref=qk_send.at[half, heads], dst_ref=q_all.at[half, :, half_rows(half, owner), :])

    def exchange(make, send, recv, peer):
        @pl.when(peer != inner)
        def _():
            for half in range(2):
                refs = make(half, peer, inner)
                pltpu.make_async_remote_copy(send_sem=send.at[half, peer], recv_sem=recv.at[half, inner],
                                             device_id=across(peer), device_id_type=MESH, **refs).start()

        @pl.when(peer == inner)
        def _():
            for half in range(2):
                refs = make(half, peer, inner)
                pltpu.make_async_copy(refs["src_ref"], refs["dst_ref"], recv.at[half, inner]).start()

    def k_landed(src, _):
        for half in range(2):
            landed(k_all.at[half_block(half, outer), half_rows(half, src), :], recv_k.at[half, src])
        return 0

    def v_landed(src, _):
        for half in range(2):
            landed(v_all.at[half_block(half, outer), :, half_rows(half, src)], recv_v.at[half, src])
        return 0

    def y_parts(src):
        return (k_all.at[src], k_all.at[mirror - src], v_all.at[src], v_all.at[mirror - src])

    def y_send(src, part, slot, lane, peer):
        ref = y_parts(src)[part]
        return pltpu.make_async_remote_copy(src_ref=ref, dst_ref=ref, send_sem=send_y.at[slot, part],
                                            recv_sem=recv_y.at[lane, part], device_id=along(peer), device_id_type=MESH)

    def project(w_buf):
        def group_of(n):
            return beyond(jnp.where(n == 0, 1, jnp.where(n == 1, groups - 1, jnp.where(n == 2, 2, 0))))

        def fetch_q(n, slot):
            heads = pl.ds(pl.multiple_of(group_of(n) * n_inner, n_inner), n_inner)
            return pltpu.make_async_copy(wq_ref.at[:, heads, :], w_buf.at[slot], w_sem.at[slot])

        fetch_k = pltpu.make_async_copy(wk_ref, w_buf.at[0], w_sem.at[0])
        fetch_v = pltpu.make_async_copy(wv_ref, w_buf.at[1], w_sem.at[1])
        fetch_x = pltpu.make_async_copy(x_hbm, x_ref, w_sem.at[2])
        fetch_x.start()
        fetch_k.start()
        pl.semaphore_wait(barrier, n_inner + 1)

        def product(slot):
            return jnp.dot(x_ref[...], w_buf[slot].reshape(model, n_inner * hd), preferred_element_type=F32)

        def rotate_store(y_all, base):
            for h in range(n_inner):
                y = y_all[:, h * hd:(h + 1) * hd]
                r = (y * cos_ref[...] + pltpu.roll(y, hd // 2, 1) * sin_ref[...]).astype(BF16)
                for half in range(2):
                    qk_send[half, base + h] = r[half * chunk:(half + 1) * chunk]

        def to_all(make, send, recv):
            def one(d, _):
                exchange(make, send, recv, lax.rem(inner + d, n_inner))
                return 0
            lax.fori_loop(0, n_inner, one, 0)

        fetch_x.wait()
        fetch_k.wait()
        fetch_v.start()
        rotate_store(product(0), 0)
        to_all(k_copy, send_k, recv_k)

        fetch_v.wait()
        fetch_q(0, 0).start()
        y_all = product(1)
        for h in range(n_inner):
            vt = y_all[:, h * hd:(h + 1) * hd].T.astype(BF16)
            for half in range(2):
                v_send[half, h] = vt[:, half * chunk:(half + 1) * chunk]
        fetch_q(1, 1).start()
        to_all(v_copy, send_v, recv_v)

        def step(n, _):
            slot = lax.rem(n, 2)
            fetch_q(n, slot).wait()
            first = group_of(n)
            rotate_store(product(slot), n_inner + first * n_inner)

            @pl.when(n + 2 < groups)
            def _():
                fetch_q(n + 2, slot).start()

            def one(d, _):
                exchange(q_copy, send_q, recv_q, first * (n_inner // groups) + d)
                return 0
            lax.fori_loop(0, n_inner // groups, one, 0)

            for when, here_yet, parts in ((1, k_landed, (0, 1)), (groups - 1, v_landed, (2, 3))):
                @pl.when(n == when)
                def _():
                    lax.fori_loop(0, n_inner, here_yet, 0)
                    for part in parts:
                        y_send(outer, part, 0, 0, up).start()
                        y_send(outer, part, 1, 1, down).start()
            return 0
        lax.fori_loop(0, groups, step, 0)

    pl.run_scoped(project, pltpu.VMEM((2, model, n_inner, hd), BF16))

    def attend(w_buf, total, s0, s1, qt, m_buf, l_buf, acc):
        deep = w_buf.shape[1]

        def out_chip(c):
            return beyond(jnp.where(c == 1, 2, jnp.where(c == 2, 1, jnp.where(c == 3, groups - 1, 0))))

        def out_weights(c, slot):
            rows_of = pl.ds(pl.multiple_of(out_chip(c) * deep, deep), deep)
            return pltpu.make_async_copy(wo_ref.at[rows_of, :], w_buf.at[slot], w_sem.at[slot])

        for c in range(2):
            out_weights(c, c).start()

        def qk(s_buf, unit):
            side, t, kb, part_of = unit
            if part_of is None:
                s_buf[...] = jnp.dot(k_all[kb], qt[side * n_tiles + t], preferred_element_type=F32)
            else:
                keys = pl.ds(pl.multiple_of(part_of * piece, piece), piece)
                s_buf[:piece] = jnp.dot(k_all[kb, keys, :], qt[side * n_tiles + t], preferred_element_type=F32)

        def soft(s_buf, unit):
            side, t, kb, part_of = unit
            idx = side * n_tiles + t
            if part_of is None:
                s, v = s_buf[...], v_all[kb]
            else:
                keys = pl.ds(pl.multiple_of(part_of * piece, piece), piece)
                s, v = s_buf[:piece], v_all[kb, :, keys]
                key = lax.broadcasted_iota(jnp.int32, s.shape, 0) + (part_of * piece - t * tile)
                pos = lax.rem(lax.broadcasted_iota(jnp.int32, s.shape, 1), tile)
                s = jnp.where(key <= pos, s, NEG_BIG)
            m_old = m_buf[idx]
            m_new = jnp.maximum(m_old, s.max(axis=0, keepdims=True))
            p = jnp.exp2((s - m_new) * scale)
            rescale = jnp.exp2((m_old - m_new) * scale)
            m_buf[idx] = m_new
            l_buf[idx] = l_buf[idx] * rescale + p.sum(axis=0, keepdims=True)
            acc[idx] = acc[idx] * rescale + jnp.dot(v, p.astype(BF16), preferred_element_type=F32)

        def run(units):
            bufs = (s0, s1)
            qk(bufs[0], units[0])
            for n, unit in enumerate(units):
                if n + 1 < len(units):
                    qk(bufs[(n + 1) % 2], units[n + 1])
                soft(bufs[n % 2], unit)

        def own(step, _):
            chip = beyond(jnp.where(step == 2, 3, jnp.where(step == 3, 2, step)))
            t_side = (chip, n_tiles - 1 - chip)

            @pl.when(step == 2)
            def _():
                for part in (0, 1):
                    landed(y_parts(down)[part], recv_y.at[0, part])
                    y_send(down, part, 2, 2, up).start()

            def q_landed(src, _):
                for half in range(2):
                    landed(q_all.at[half, :, half_rows(half, src), :], recv_q.at[half, src])
                return 0
            lax.fori_loop(chip * (n_inner // groups), (chip + 1) * (n_inner // groups), q_landed, 0)

            for side in range(2):
                t = t_side[side]
                idx = side * n_tiles + t
                for h in range(per_kv):
                    q_tile = q_all[side, h, pl.ds(pl.multiple_of(t * tile, tile), tile), :]
                    qt[idx, :, h * tile:(h + 1) * tile] = q_tile.T
                m_buf[idx] = jnp.full((1, cols), NEG_BIG, F32)
                l_buf[idx] = jnp.zeros((1, cols), F32)
                acc[idx] = jnp.zeros((hd, cols), F32)
            units = []
            for n in range(n_tiles // 2 + 1):
                last_front = chip * tile // piece
                front = n <= last_front
                units.append((jnp.where(front, 0, 1), jnp.where(front, t_side[0], t_side[1]),
                              jnp.where(front, outer, mirror - outer), jnp.where(front, n, n - last_front - 1)))
            run(units + [(1, t_side[1], outer, None)])
            return 0
        lax.fori_loop(0, n_tiles, own, 0)

        for part in (2, 3):
            landed(y_parts(up)[part], recv_y.at[1, part])
            y_send(up, part, 2, 2, down).start()
        for part in (0, 1):
            landed(y_parts(up)[part], recv_y.at[1, part])
        for part in (2, 3):
            landed(y_parts(down)[part], recv_y.at[0, part])

        def source(src, t_side):
            earlier = src < outer
            return [(jnp.where(earlier, 0, 1), jnp.where(earlier, t_side[0], t_side[1]), src, None),
                    (1, t_side[1], jnp.where(earlier, src, mirror - src), None)]

        def o_copy(half, t, j):
            c = 2 * t + j
            peer = c if half == 0 else n_inner - 1 - c
            src = o_stage.at[half, t, pl.ds(j * chunk, chunk), :]
            dst = o_all.at[pl.ds(half * chunk, chunk), pl.ds(pl.multiple_of(inner * per_kv * hd, per_kv * hd), per_kv * hd)]
            return peer, src, dst

        def by_distance(step):
            return beyond(jnp.where(step == 0, 2, jnp.where(step == 1, 1, jnp.where(step == 2, groups - 1, 0))))

        def neighbours(step, _):
            chip = by_distance(step)
            t_side = (chip, n_tiles - 1 - chip)
            run(source(down, t_side) + source(up, t_side))
            return 0
        lax.fori_loop(0, 2, neighbours, 0)

        for part in range(4):
            landed(y_parts(far)[part], recv_y.at[2, part])

        def last(step, _):
            chip = by_distance(step)
            t_side = (chip, n_tiles - 1 - chip)

            @pl.when(step >= 2)
            def _():
                run(source(down, t_side) + source(up, t_side))

            run(source(far, t_side))
            for half in range(2):
                t = t_side[half]
                idx = half * n_tiles + t
                o_t = acc[idx] / l_buf[idx]
                for h in range(per_kv):
                    o_stage[half, t, :, h * hd:(h + 1) * hd] = o_t[:, h * tile:(h + 1) * tile].T.astype(BF16)
                for j in range(2):
                    peer, src, dst = o_copy(half, t, j)

                    @pl.when(peer != inner)
                    def _():
                        pltpu.make_async_remote_copy(src_ref=src, dst_ref=dst, send_sem=send_o.at[half, peer],
                                                     recv_sem=recv_o.at[half, inner], device_id=across(peer),
                                                     device_id_type=MESH).start()

                    @pl.when(peer == inner)
                    def _():
                        pltpu.make_async_copy(src, dst, recv_o.at[half, inner]).start()
            return 0
        lax.fori_loop(0, n_tiles, last, 0)

        def o_landed(src, _):
            for half in range(2):
                landed(o_all.at[pl.ds(half * chunk, chunk), pl.ds(pl.multiple_of(src * per_kv * hd, per_kv * hd), per_kv * hd)],
                       recv_o.at[half, src])
            return 0

        def out_step(c, _):
            slot = lax.rem(c, 2)
            chip = out_chip(c)
            per_chip = n_inner // groups
            lax.fori_loop(chip * per_chip, (chip + 1) * per_chip, o_landed, 0)
            out_weights(c, slot).wait()
            here_cols = pl.ds(pl.multiple_of(chip * deep, deep), deep)
            part = jnp.dot(o_all[:, here_cols], w_buf[slot], preferred_element_type=F32)

            @pl.when(c == 0)
            def _():
                total[...] = part

            @pl.when(c > 0)
            def _():
                total[...] += part

            @pl.when(c + 2 < groups)
            def _():
                out_weights(c + 2, slot).start()
            return 0
        lax.fori_loop(0, groups, out_step, 0)
        out_ref[...] = total[...].astype(BF16)

        def sent(d, _):
            peer = lax.rem(inner + d, n_inner)
            heads = pl.ds(n_inner + peer * per_kv, per_kv)
            for half in range(2):
                landed(qk_send.at[half, peer], send_k.at[half, peer])
                landed(v_send.at[half, peer], send_v.at[half, peer])
                landed(qk_send.at[half, heads], send_q.at[half, peer])
                landed(o_stage.at[half, 0, pl.ds(0, chunk), :], send_o.at[half, peer])
            return 0
        lax.fori_loop(1, n_inner, sent, 0)
        for slot in range(3):
            for part in range(4):
                landed(y_parts(outer)[part], send_y.at[slot, part])

    pl.run_scoped(attend, pltpu.VMEM((2, wo_ref.shape[0] // groups, model), BF16), pltpu.VMEM((rows, model), F32), pltpu.VMEM((block, cols), F32),
                  pltpu.VMEM((block, cols), F32), pltpu.VMEM((2 * n_tiles, hd, cols), BF16),
                  pltpu.VMEM((2 * n_tiles, 1, cols), F32), pltpu.VMEM((2 * n_tiles, 1, cols), F32),
                  pltpu.VMEM((2 * n_tiles, hd, cols), F32))


def solution(mesh):
    n_outer = mesh.shape['cpo']
    n_inner = mesh.shape['cpi']
    n_dev = n_outer * n_inner

    def device_step(hidden, w_query, w_key, w_value, w_out):
        rows, model = hidden.shape
        chunk = rows // 2
        q_heads, hd = w_query.shape[1:]
        per_kv = q_heads // n_inner
        block = n_inner * chunk
        n_tiles = block // (2 * chunk)
        rank = lax.axis_index('cpo') * n_inner + lax.axis_index('cpi')
        offsets = jnp.arange(chunk, dtype=jnp.int32)
        positions = jnp.concatenate([rank * chunk + offsets, (2 * n_dev - 1 - rank) * chunk + offsets])
        cos, sin = rope_tables(positions, hd)
        dma = pltpu.SemaphoreType.DMA
        pair = dma((2, n_inner))
        vmem = pl.BlockSpec(memory_space=pltpu.VMEM)
        hbm = pl.BlockSpec(memory_space=pl.ANY)
        return pl.pallas_call(
            functools.partial(layer_kernel, n_outer, n_inner),
            out_shape=jax.ShapeDtypeStruct((rows, model), BF16),
            in_specs=[hbm] + [vmem] * 2 + [hbm] * 4,
            out_specs=vmem,
            scratch_shapes=[
                pltpu.VMEM((rows, model), BF16),
                pltpu.VMEM((2, n_inner + q_heads, chunk, hd), BF16),
                pltpu.VMEM((2, n_inner, hd, chunk), BF16),
                pltpu.VMEM((2 * n_outer, block, hd), BF16),
                pltpu.VMEM((2 * n_outer, hd, block), BF16),
                pltpu.VMEM((2, per_kv, block, hd), BF16),
                pltpu.VMEM((2, n_tiles, 2 * chunk, per_kv * hd), BF16),
                pltpu.VMEM((rows, q_heads * hd), BF16),
                dma((3,)), pair, pair, pair, pair, pair, pair, pair, pair, dma((3, 4)), dma((3, 4)),
            ],
            compiler_params=pltpu.CompilerParams(collective_id=0, has_side_effects=True, vmem_limit_bytes=62 * 1024 * 1024),
        )(hidden, cos, sin, w_query, w_key, w_value, w_out.reshape(q_heads * hd, model))

    row_spec = P(('dp', 'cpo', 'cpi'), None)
    weight_spec = P(None, None, None)
    return jax.shard_map(device_step, mesh=mesh, in_specs=(row_spec, weight_spec, weight_spec, weight_spec, weight_spec), out_specs=row_spec, check_vma=False)
```
